512 devices in a mesh: dp: 8 (over x, core), expert: 64 (over y, z).
Axes of the slice: x: 4, y: 8, z: 8, core: 2. Of those that a mesh axis runs over, the one named last changes fastest.
Arguments:
- cotangent: bfloat16 [65536, 3584], P(('dp', 'expert')), may hold values from -0.59765625 to 0.59765625
- expert_ids: int32 [65536, 1], P(('dp', 'expert')), may hold values from 0 to 15; in each aligned block of 128 rows (0 to 127, 128 to 255, ...) at most 12 rows name the same one
- route_weights: float32 [65536, 1], P(('dp', 'expert')), may hold values from 0.1 to 1
- gate_pre: bfloat16 [6144, 16384], P('dp', 'expert'), may hold values from -5 to 5
- up_pre: bfloat16 [6144, 16384], P('dp', 'expert'), may hold values from -5 to 5
- down_weight: bfloat16 [3584, 16384], P('dp', 'expert'), may hold values from -0.1875 to 0.1875
Outputs:
- weight_grad: bfloat16 [3584, 16384], P('dp', 'expert')
- gate_grad: bfloat16 [6144, 16384], P('dp', 'expert')
- up_grad: bfloat16 [6144, 16384], P('dp', 'expert')
The draws below stay inside these ranges and needn't reach their ends.
Inputs may be any that keep to these rules, and one draw needn't show every extreme that they name: `expert_ids`: each token names one expert. Among the tokens of one device, at most 12 name the same expert, and in every draw some expert is named by exactly 12 tokens of some device.
All inputs are finite; a program needn't handle non-finite values.
Results may differ from the reference program's by a relative error of at most 0.013.
Values may be sent and summed in bfloat16 or wider, within the bound.
A program may use at most 64 MiB of HBM per device.

```python
import math
import jax
import jax.numpy as jnp
import numpy as np
from jax import lax

D = 3584
FFW = 1024
TOP = 1
TOK_DEV = 128
EXPERTS = 16
CAP = 12
TOKENS = 65536
SLOTS = 6144
N_DP = 8
N_EXPERT = 64


def shard_levels(own_key, extent, split, low, largest):
    def one(axis_at, parts):
        steps = jax.random.uniform(jax.random.fold_in(jax.random.fold_in(own_key, 6), axis_at), (parts,), jnp.float32, low / len(split), largest / len(split))
        return jnp.repeat(jnp.exp(steps), extent[axis_at] // parts).reshape((-1,) + (1,) * (len(extent) - axis_at - 1))

    gain = one(*split[0])
    for cut in split[1:]:
        gain = gain * one(*cut)
    return gain


def assign_block(own_key, own, number, rows, count, top, limit, skew):
    order = jax.random.permutation(own_key, count)
    heavy_load, common = load_shares(count, rows * top, limit, skew, True), load_shares(count, rows * top, limit, skew, False)
    places = jnp.arange(count)

    def named(lengths, turn):
        used = int((lengths > 0).sum())
        fixed = max(1, used // 4)
        shifted = fixed + (places - fixed + turn * (used - fixed)) % max(1, count - fixed)
        return jnp.zeros((count,), jnp.int32).at[order[jnp.where(places < fixed, places, shifted)]].set(jnp.asarray(lengths, jnp.int32))

    lengths = jnp.where(number % 4 == 0, named(heavy_load, number // 4), named(common, number - number // 4 - 1))
    mixed = jax.random.permutation(jax.random.fold_in(own, 3), count)
    source_of, receiver = mixed[0:count // 2 * 2:2], mixed[1:count // 2 * 2:2]
    room = jnp.minimum(lengths[source_of] - 1, limit - lengths[receiver]) // 2
    room = jnp.where((source_of == order[0]) | (receiver == order[0]) | (lengths[receiver] == 0), 0, jnp.maximum(room, 0))
    shifted = jax.random.randint(jax.random.fold_in(own, 4), (count // 2,), 0, 1 << 20) % (room + 1)
    lengths = lengths.at[source_of].add(-shifted).at[receiver].add(shifted)
    labels = jnp.searchsorted(jnp.cumsum(lengths), jnp.arange(rows * top), side="right").astype(jnp.int32)
    listing = labels.reshape(top, rows).T
    listing = listing[jax.random.permutation(jax.random.fold_in(own, 1), rows)]
    turn = jax.random.randint(jax.random.fold_in(own, 2), (rows, 1), 0, top)
    return jnp.take_along_axis(listing, (jnp.arange(top)[None, :] + turn) % top, axis=1)


def load_shares(count, total, most, lean, full):
    weights = [(1 << 20) // math.isqrt(standing ** lean) + 1 for standing in range(1, count + 1)]
    largest = most if full else min(most, max(-(-total // count), total * weights[0] // sum(weights)))
    least = 1 if total - largest >= count - 1 else 0
    holding, surplus = [largest] + [least] * (count - 1), total - largest - least * (count - 1)
    while surplus > 0:
        movable = [i for i in range(1, count) if holding[i] < largest] or [i for i in range(1, count) if holding[i] < most]
        whole, left = sum([weights[i] for i in movable]), surplus
        for i in movable:
            more = min(most - holding[i], max(1, left * weights[i] // whole), surplus)
            holding[i] = holding[i] + more
            surplus = surplus - more
    return np.array(holding)


def normal_values(rng, extent, width, limit, cuts=(), kind=jnp.bfloat16):
    drawn = width * jax.random.normal(rng, extent, jnp.float32)
    if cuts:
        drawn = drawn * shard_levels(rng, extent, cuts, -0.22, 0.18)
    return jnp.clip(drawn, -limit, limit).astype(kind)


def setup_inputs(seed: int = 0) -> dict:
    splits = jax.random.split(jax.random.key(seed), 7)
    cotangent = normal_values(splits[0], (TOKENS, D), 0.1, 0.59765625, ((0, 512),))
    expert_ids_keys = jax.random.split(jax.random.fold_in(splits[1], 1), TOKENS // TOK_DEV)
    expert_ids_turns = jax.random.permutation(jax.random.fold_in(splits[1], 3), TOKENS // TOK_DEV)
    expert_ids = jax.vmap(lambda own, number: assign_block(jax.random.fold_in(splits[1], 2), own, number, TOK_DEV, EXPERTS, TOP, CAP, 2))(expert_ids_keys, expert_ids_turns).reshape((TOKENS, TOP))
    route_weights = jnp.clip(0.1 + 0.9 * jax.random.uniform(splits[2], (TOKENS, TOP), jnp.float32) ** shard_levels(splits[2], (TOKENS, TOP), ((0, 512),), -0.2, 0.2), 0.1, 1.0)
    gate_pre = normal_values(splits[3], (SLOTS, EXPERTS * FFW), 1.0, 5.0, ((0, 8), (1, 64)))
    up_pre = normal_values(splits[4], (SLOTS, EXPERTS * FFW), 1.0, 5.0, ((0, 8), (1, 64)))
    down_weight = normal_values(splits[5], (D, EXPERTS * FFW), FFW ** -0.5, 0.1875, ((0, 8), (1, 64)))
    return {"cotangent": cotangent, "expert_ids": expert_ids, "route_weights": route_weights, "gate_pre": gate_pre, "up_pre": up_pre, "down_weight": down_weight}


def group_terms(cotangent, expert_ids, route_weights, gate_pre, up_pre, down_weight):
    onehot = (expert_ids[..., None] == jnp.arange(EXPERTS, dtype=jnp.int32)).astype(jnp.int32)
    touched = jnp.sum(onehot, axis=2)
    earlier = jnp.cumsum(touched, axis=1) - touched
    position = jnp.sum(onehot * earlier[:, :, None, :], axis=3)
    sources = jnp.arange(N_EXPERT, dtype=jnp.int32)[:, None, None] * CAP
    rows = (sources + position).astype(jnp.int32)
    scaled = route_weights[..., None] * cotangent.astype(jnp.float32)[:, :, None, :]
    routed = jnp.zeros((EXPERTS, N_EXPERT * CAP, D), jnp.float32).at[expert_ids, rows].add(scaled)
    routed_half = lax.optimization_barrier(routed.astype(jnp.bfloat16))
    routed_full = routed_half.astype(jnp.float32)
    weights = down_weight.astype(jnp.float32).reshape(D, EXPERTS, FFW)
    gate_full = gate_pre.astype(jnp.float32).reshape(N_EXPERT * CAP, EXPERTS, FFW)
    up_full = up_pre.astype(jnp.float32).reshape(N_EXPERT * CAP, EXPERTS, FFW)
    upstream = jnp.einsum('xrd,dxf->rxf', routed_full, weights)
    sigmoid = jax.nn.sigmoid(gate_full)
    active = gate_full * sigmoid
    product_half = lax.optimization_barrier((active * up_full).astype(jnp.bfloat16))
    gate_grad = (upstream * up_full * sigmoid * (1.0 + gate_full * (1.0 - sigmoid))).astype(jnp.bfloat16)
    up_grad = (upstream * active).astype(jnp.bfloat16)
    partial_sum = jnp.einsum('xrd,rxf->dxf', routed_full, product_half.astype(jnp.float32))
    partial_half = partial_sum.reshape(D, EXPERTS * FFW).astype(jnp.bfloat16)
    return partial_half, gate_grad.reshape(N_EXPERT * CAP, EXPERTS * FFW), up_grad.reshape(N_EXPERT * CAP, EXPERTS * FFW)


def reference(cotangent, expert_ids, route_weights, gate_pre, up_pre, down_weight):
    stacked = (cotangent.reshape(N_DP, N_EXPERT, TOK_DEV, D),
               expert_ids.reshape(N_DP, N_EXPERT, TOK_DEV, TOP),
               route_weights.reshape(N_DP, N_EXPERT, TOK_DEV, TOP),
               gate_pre.reshape(N_DP, N_EXPERT * CAP, EXPERTS * FFW),
               up_pre.reshape(N_DP, N_EXPERT * CAP, EXPERTS * FFW))

    def step(total, pieces):
        partial_half, gate_grad, up_grad = group_terms(pieces[0], pieces[1], pieces[2], pieces[3], pieces[4], down_weight)
        return total + partial_half.astype(jnp.float32), (gate_grad, up_grad)

    start = jnp.zeros((D, EXPERTS * FFW), jnp.float32)
    total, grads = lax.scan(step, start, stacked)
    weight_grad = total.astype(jnp.bfloat16)
    gate_grad = grads[0].reshape(SLOTS, EXPERTS * FFW)
    up_grad = grads[1].reshape(SLOTS, EXPERTS * FFW)
    return weight_grad, gate_grad, up_grad
```

```python
import functools

import jax
import jax.numpy as jnp
from jax import lax
from jax.experimental import pallas as pl
from jax.experimental.pallas import tpu as pltpu
from jax.sharding import PartitionSpec as P

LANES = 4
NZ = 8
GROUPS = 4
WIDTH = 128
SUB = 64


def kernel(
    sizes,
    cot_hbm,
    ids_hbm,
    weights_hbm,
    gate_hbm,
    up_hbm,
    down_hbm,
    wgrad_ref,
    ggrad_ref,
    ugrad_ref,
    cot_ref,
    ids_ref,
    weights_ref,
    gate_ref,
    up_ref,
    load,
    blocks,
    scale,
    sendbuf,
    over_y,
    over_z,
    down,
    slope,
    active,
    perm,
    order,
    product,
    product_in,
    products,
    rows,
    upstream,
    up_mine,
    up_out,
    grads,
    grads_in,
    reduced,
    reduced_in,
    kept,
    half_out,
    half_in,
    y_send,
    y_recv,
    z_send,
    z_recv,
    wz_send,
    wz_recv,
    wx_send,
    wx_recv,
    wc_send,
    wc_recv,
    p_send,
    p_recv,
    u_send,
    u_recv,
    g_send,
    g_recv,
    r_send,
    r_recv,
    o_send,
    o_recv,
):
    n, ny, cap, chunks, quarter = sizes
    nx = n // 2
    experts = 2 * ny
    tokens = ids_ref.shape[1]
    hidden = gate_ref.shape[1]
    slab = GROUPS * cap
    zrows = ny * cap
    half, full = jnp.bfloat16, jnp.float32

    dp = lax.axis_index("dp")
    me = lax.axis_index("expert")
    x, core = dp // 2, dp % 2
    y, z = me // NZ, me % NZ
    side = z // LANES
    pair = z // 2
    inner = 2 * pair + pair % 2
    is_inner = z == inner
    near_z = z + 1 - 2 * (z % 2)
    across_z = NZ - 1 - inner
    outer_z = across_z + 1 - 2 * (across_z % 2)
    partner_z = z - z % LANES + (z % LANES + 2) % LANES
    partner_pair = partner_z // 2
    slots = (z, near_z, across_z, outer_z)
    sibling = {"dp": x * 2 + 1 - core}
    near = {"expert": y * NZ + near_z}
    across = {"expert": y * NZ + across_z}
    partner = {"expert": y * NZ + partner_z}
    far_slot = jnp.where(is_inner, 1, 2)

    def at_y(k):
        return {"expert": (y + k) % ny * NZ + z}

    def at_x(k):
        return {"dp": (x + k) % nx * 2 + core}

    mine_rows = pl.ds(chunks * core, chunks)
    loads = [
        pltpu.make_async_copy(source, to, load.at[i])
        for i, (source, to) in enumerate(
            (
                (ids_hbm, ids_ref),
                (weights_hbm, weights_ref),
                (cot_hbm, cot_ref),
                (down_hbm, down.at[0, x, mine_rows]),
                (gate_hbm, gate_ref),
                (up_hbm, up_ref),
            )
        )
    ]
    for copy in loads:
        copy.start()

    barrier = pltpu.get_barrier_semaphore()

    def greet(target):
        pl.semaphore_signal(
            barrier, inc=1, device_id=target, device_id_type=pl.DeviceIdType.MESH
        )

    for k in range(1, ny):
        greet(at_y(k))
    greet(near)
    greet(across)
    greet({"expert": y * NZ + outer_z})
    greet(partner)
    for k in range(1, n):
        greet({"dp": (dp + k) % n})
    greeted = ny - 1 + 4 + n - 1

    def send(source, to, sent, arrived, device):
        pltpu.make_async_remote_copy(
            src_ref=source,
            dst_ref=to,
            send_sem=sent,
            recv_sem=arrived,
            device_id=device,
            device_id_type=pl.DeviceIdType.MESH,
        ).start()

    def await_bytes(ref_at, sem):
        pltpu.make_async_copy(ref_at, ref_at, sem).wait()

    def steps_of(index, step, count):
        total = jnp.zeros_like(index)
        for k in range(1, count):
            total = total + jnp.where(index >= k * step, 1, 0)
        return total

    loads[0].wait()
    loads[1].wait()
    ids_row, weight_row = ids_ref[...], weights_ref[...]
    first = lax.broadcasted_iota(jnp.int32, (tokens, tokens), 0)
    second = lax.broadcasted_iota(jnp.int32, (tokens, tokens), 1)
    names = lax.broadcasted_iota(jnp.int32, (experts, tokens), 0) == ids_row
    before = jnp.where(first < second, 1.0, 0.0).astype(half)
    earlier = jnp.dot(jnp.where(names, 1.0, 0.0).astype(half), before, preferred_element_type=full)
    position = jnp.sum(jnp.where(names, earlier, 0.0), axis=0, keepdims=True).astype(jnp.int32)
    target = ids_row * cap + position
    shape = (experts, slab, tokens)
    inside = lax.broadcasted_iota(jnp.int32, shape, 1)
    group = steps_of(inside, cap, GROUPS)
    slot = lax.broadcasted_iota(jnp.int32, shape, 0) * cap + inside - group * cap
    slot = slot.reshape(experts * slab, tokens)
    group = group.reshape(experts * slab, tokens)
    chosen = slot == target
    scale[...] = jnp.sum(jnp.where(chosen, weight_row, 0.0), axis=1, keepdims=True)
    for g in range(GROUPS):
        blocks[:, g * tokens : (g + 1) * tokens] = jnp.where(chosen & (group == g), 1.0, 0.0).astype(half)

    def pick(j):
        columns = jnp.concatenate(
            [
                cot_ref[:, pl.ds(pl.multiple_of(g * quarter + j * WIDTH, WIDTH), WIDTH)]
                for g in range(GROUPS)
            ],
            axis=0,
        )
        picked = jnp.dot(blocks[...], columns, preferred_element_type=full) * scale[...]
        sendbuf[j] = picked.astype(half).reshape(ny, 2, slab, WIDTH)
        for s in range(2):
            over_y[j, s, y] = sendbuf[j, y, s]

    def send_y(j):
        for k in range(1, ny):
            send(
                sendbuf.at[j, (y + k) % ny], over_y.at[j, :, y], y_send.at[j], y_recv.at[j], at_y(k)
            )

    def down_at(f, k):
        return down.at[f, (x - k + nx) % nx, mine_rows]

    def down_other(f, k):
        return down.at[f, (x - k + nx) % nx, pl.ds(chunks * (1 - core), chunks)]

    def send_down_x(f):
        for k in range(1, nx):
            send(down_at(f, 0), down_at(f, 0), wx_send.at[f, k - 1], wx_recv.at[f, k - 1], at_x(k))

    def send_down_core(f, k):
        send(down_at(f, k), down_at(f, k), wc_send.at[f, k], wc_recv.at[f, k], sibling)

    loads[2].wait()
    pick(0)
    loads[3].wait()
    pl.semaphore_wait(barrier, greeted)
    send(down_at(0, 0), down_at(1, 0), wz_send, wz_recv, partner)
    send_y(0)
    send_down_x(0)
    send_down_core(0, 0)

    @pl.loop(1, chunks)
    def _(j):
        pick(j)
        send_y(j)

    @pl.loop(0, NZ)
    def _(a):
        shape = (zrows, NZ * zrows)
        at = lax.broadcasted_iota(jnp.int32, shape, 0)
        b = steps_of(at, cap, ny)
        source = b * zrows + a * cap + at - b * cap
        hit = lax.broadcasted_iota(jnp.int32, shape, 1) == source
        perm[a] = jnp.where(hit, 1.0, 0.0).astype(half)

    loads[4].wait()
    loads[5].wait()

    @pl.loop(0, NZ)
    def _(i):
        at = pl.ds(pl.multiple_of(i * zrows, 16), zrows)
        gate = gate_ref[at, :].astype(full)
        up = up_ref[at, :].astype(full)
        sig = jax.nn.sigmoid(gate)
        act = gate * sig
        active[at, :] = act
        slope[at, :] = up * sig * (1.0 + gate * (1.0 - sig))
        gate_ref[at, :] = (act * up).astype(half)

    @pl.loop(0, NZ)
    def _(a):
        product[a] = jnp.dot(perm[a], gate_ref[...], preferred_element_type=full).astype(half)

    def halves(p):
        return pl.ds(2 * p, 2)

    theirs = (partner_pair, NZ // 2 - 1 - partner_pair)
    ours = (pair, NZ // 2 - 1 - pair)
    for i in range(2):
        send(
            product.at[halves(theirs[i])],
            product_in.at[halves(theirs[i])],
            p_send.at[i],
            p_recv.at[i],
            partner,
        )
    await_bytes(down_at(1, 0), wz_recv)
    send_down_x(1)
    send_down_core(1, 0)

    spread = (zrows, ny * slab)
    for g in range(GROUPS):
        at = lax.broadcasted_iota(jnp.int32, spread, 0)
        b = steps_of(at, cap, ny)
        source = b * slab + g * cap + at - b * cap
        hit = lax.broadcasted_iota(jnp.int32, spread, 1) == source
        order[g * zrows : (g + 1) * zrows, :] = jnp.where(hit, 1.0, 0.0).astype(half)
    upstream[...] = jnp.zeros_like(upstream)

    def send_z(j):
        await_bytes(over_y.at[j, :, pl.ds(0, ny - 1)], y_recv.at[j])
        send(
            over_y.at[j, 1 - side], over_z.at[j, far_slot], z_send.at[j, 1], z_recv.at[j, far_slot], across
        )
        send(over_y.at[j, side], over_z.at[j, 0], z_send.at[j, 0], z_recv.at[j, 0], near)

    def forward(j):
        @pl.when(is_inner)
        def _():
            for s in (1, 2):
                await_bytes(over_z.at[j, s], z_recv.at[j, s])
                send(over_z.at[j, s], over_z.at[j, s], z_send.at[j, s + 1], z_recv.at[j, s], near)

    def forward_down():
        for f in range(2):
            for k in range(1, nx):
                await_bytes(down_at(f, k), wx_recv.at[f, k - 1])
                send_down_core(f, k)

    def gather_products():
        for i in range(2):
            await_bytes(product_in.at[halves(ours[i])], p_recv.at[i])
        for s in range(4):
            at = slice(s * zrows, (s + 1) * zrows)
            products[at, :hidden] = product[slots[s]]
            products[at, hidden:] = product_in[slots[s]]

    def await_down():
        for f in range(2):
            for k in range(nx):
                await_bytes(down_other(f, k), wc_recv.at[f, k])

    def compute(j):
        await_bytes(over_z.at[j, 0], z_recv.at[j, 0])

        @pl.when(jnp.logical_not(is_inner))
        def _():
            for s in (1, 2):
                await_bytes(over_z.at[j, s], z_recv.at[j, s])

        raw = jnp.concatenate(
            [over_y[j, side].reshape(ny * slab, WIDTH)]
            + [over_z[j, s].reshape(ny * slab, WIDTH) for s in range(3)],
            axis=1,
        )
        sorted_rows = jnp.dot(order[...], raw, preferred_element_type=full).astype(half)
        for s in range(4):
            for g in range(GROUPS):
                rows[s * zrows : (s + 1) * zrows, g * WIDTH : (g + 1) * WIDTH] = sorted_rows[
                    g * zrows : (g + 1) * zrows, s * WIDTH : (s + 1) * WIDTH
                ]
        for f in range(2):
            columns = slice(f * hidden, (f + 1) * hidden)
            grad = lax.dot_general(
                rows[...], products[:, columns], (((0,), (0,)), ((), ())), preferred_element_type=full
            )
            grads[j, :, :, :, columns] = grad.astype(half).reshape(GROUPS, 2, SUB, hidden)
        for k in range(2):
            send(grads.at[j, 2 * k + 1 - core], grads_in.at[j, k], g_send.at[j, k], g_recv.at[j, k], sibling)
        for f in range(2):
            columns = slice(f * hidden, (f + 1) * hidden)
            weights = down[f, :, pl.ds(2 * j, 2)].reshape(GROUPS * WIDTH, hidden)
            upstream[:, columns] += jnp.dot(rows[...], weights, preferred_element_type=full)

    def send_upstream():
        for s in range(4):
            at = slice(s * zrows, (s + 1) * zrows)
            up_mine[slots[s]] = upstream[at, :hidden].astype(half)
            up_out[slots[s]] = upstream[at, hidden:].astype(half)
        for i in range(2):
            send(
                up_out.at[halves(ours[i])], up_mine.at[halves(ours[i])], u_send.at[i], u_recv.at[i], partner
            )

    def reduce(j):
        for k in range(2):
            await_bytes(grads_in.at[j, k], g_recv.at[j, k])
            total = grads[j, 2 * k + core].astype(full) + grads_in[j, k].astype(full)
            reduced[j, k] = total.astype(half)
            to_x = 2 * k + core
            for i in range(2):
                b = 2 * j + i
                to_core = b // chunks
                at = b % chunks
                here = (to_x == x) & (to_core == core)

                @pl.when(here)
                def _():
                    pltpu.make_async_copy(
                        reduced.at[j, k, i], reduced_in.at[x, at], r_recv.at[x, at]
                    ).start()

                @pl.when(jnp.logical_not(here))
                def _():
                    send(
                        reduced.at[j, k, i],
                        reduced_in.at[x, at],
                        r_send.at[j, k, i],
                        r_recv.at[x, at],
                        {"dp": to_x * 2 + to_core},
                    )

    def owned(j, act):
        for i in range(2):
            b = 2 * j + i

            @pl.when(b // chunks == core)
            def _():
                act(b % chunks)

    def combine(at):
        total = jnp.zeros((SUB, 2 * hidden), full)
        for s in range(nx):
            await_bytes(reduced_in.at[s, at], r_recv.at[s, at])
            total = total + reduced_in[s, at].astype(full)
        kept[at] = total[:, :hidden]
        half_out[at] = total[:, hidden:].astype(half)
        send(half_out.at[at], half_in.at[at], o_send.at[at], o_recv.at[at], partner)

    def finish(at):
        await_bytes(half_in.at[at], o_recv.at[at])
        wgrad_ref[at] = (kept[at] + half_in[at].astype(full)).astype(half)

    @pl.loop(0, chunks + 5)
    def _(t):
        @pl.when(t < chunks)
        def _():
            send_z(t)

        @pl.when((t >= 1) & (t < chunks + 1))
        def _():
            forward(t - 1)

        @pl.when(t == 1)
        def _():
            forward_down()
            gather_products()

        @pl.when(t == 2)
        def _():
            await_down()

        @pl.when((t >= 2) & (t < chunks + 2))
        def _():
            compute(t - 2)

        @pl.when((t >= 3) & (t < chunks + 3))
        def _():
            reduce(t - 3)

        @pl.when(t == chunks + 1)
        def _():
            send_upstream()

        @pl.when((t >= 4) & (t < chunks + 4))
        def _():
            owned(t - 4, combine)

        @pl.when(t >= 5)
        def _():
            owned(t - 5, finish)

    for i in range(2):
        await_bytes(up_mine.at[halves(theirs[i])], u_recv.at[i])

    @pl.loop(0, NZ)
    def _(a):
        at = pl.ds(pl.multiple_of(a * zrows, 16), zrows)
        total = jnp.dot(
            perm[a], up_mine[...].reshape(NZ * zrows, hidden), preferred_element_type=full
        )
        ggrad_ref[at, :] = (total * slope[at, :]).astype(half)
        ugrad_ref[at, :] = (total * active[at, :]).astype(half)

    await_bytes(down_at(0, 0), wz_send)
    for i in range(2):
        await_bytes(product.at[halves(theirs[i])], p_send.at[i])
        await_bytes(up_out.at[halves(ours[i])], u_send.at[i])
    for f in range(2):
        for k in range(nx):
            if k:
                await_bytes(down_at(f, 0), wx_send.at[f, k - 1])
            await_bytes(down_at(f, k), wc_send.at[f, k])

    @pl.loop(0, chunks)
    def _(j):
        await_bytes(sendbuf.at[j, pl.ds(0, ny - 1)], y_send.at[j])
        await_bytes(over_y.at[j, side], z_send.at[j, 0])
        await_bytes(over_y.at[j, 1 - side], z_send.at[j, 1])

        @pl.when(is_inner)
        def _():
            for s in (1, 2):
                await_bytes(over_z.at[j, s], z_send.at[j, s + 1])

        for k in range(2):
            await_bytes(grads.at[j, 2 * k + 1 - core], g_send.at[j, k])
            for i in range(2):

                @pl.when((2 * k + core != x) | ((2 * j + i) // chunks != core))
                def _():
                    await_bytes(reduced.at[j, k, i], r_send.at[j, k, i])

        await_bytes(half_out.at[j], o_send.at[j])


def per_device(cotangent, expert_ids, route_weights, gate_pre, up_pre, down_weight):
    n = lax.axis_size("dp")
    devices = lax.axis_size("expert")
    ny = devices // NZ
    rows, hidden = gate_pre.shape
    cap = rows // devices
    tokens, width = cotangent.shape
    depth = down_weight.shape[0]
    quarter = width // GROUPS
    chunks = quarter // WIDTH
    slab = GROUPS * cap
    zrows = ny * cap
    half, full = jnp.bfloat16, jnp.float32
    vmem = pl.BlockSpec(memory_space=pltpu.VMEM)
    anywhere = pl.BlockSpec(memory_space=pltpu.HBM)
    dma = pltpu.SemaphoreType.DMA
    weight_grad, gate_grad, up_grad = pl.pallas_call(
        functools.partial(kernel, (n, ny, cap, chunks, quarter)),
        out_shape=(
            pltpu.VMEM((chunks, SUB, hidden), half),
            pltpu.VMEM((rows, hidden), half),
            pltpu.VMEM((rows, hidden), half),
        ),
        in_specs=[anywhere] * 6,
        out_specs=(vmem, vmem, vmem),
        scratch_shapes=[
            pltpu.VMEM((tokens, width), half),
            pltpu.VMEM((1, tokens), jnp.int32),
            pltpu.VMEM((1, tokens), full),
            pltpu.VMEM((rows, hidden), half),
            pltpu.VMEM((rows, hidden), half),
            dma((6,)),
            pltpu.VMEM((2 * ny * slab, GROUPS * tokens), half),
            pltpu.VMEM((2 * ny * slab, 1), full),
            pltpu.VMEM((chunks, ny, 2, slab, WIDTH), half),
            pltpu.VMEM((chunks, 2, ny, slab, WIDTH), half),
            pltpu.VMEM((chunks, 3, ny, slab, WIDTH), half),
            pltpu.VMEM((2, n // 2, 2 * chunks, SUB, hidden), half),
            pltpu.VMEM((rows, hidden), full),
            pltpu.VMEM((rows, hidden), full),
            pltpu.VMEM((NZ, zrows, rows), half),
            pltpu.VMEM((GROUPS * zrows, ny * slab), half),
            pltpu.VMEM((NZ, zrows, hidden), half),
            pltpu.VMEM((NZ, zrows, hidden), half),
            pltpu.VMEM((4 * zrows, 2 * hidden), half),
            pltpu.VMEM((4 * zrows, GROUPS * WIDTH), half),
            pltpu.VMEM((4 * zrows, 2 * hidden), full),
            pltpu.VMEM((NZ, zrows, hidden), half),
            pltpu.VMEM((NZ, zrows, hidden), half),
            pltpu.VMEM((chunks, GROUPS, 2, SUB, 2 * hidden), half),
            pltpu.VMEM((chunks, 2, 2, SUB, 2 * hidden), half),
            pltpu.VMEM((chunks, 2, 2, SUB, 2 * hidden), half),
            pltpu.VMEM((n // 2, chunks, SUB, 2 * hidden), half),
            pltpu.VMEM((chunks, SUB, hidden), full),
            pltpu.VMEM((chunks, SUB, hidden), half),
            pltpu.VMEM((chunks, SUB, hidden), half),
            dma((chunks,)),
            dma((chunks,)),
            dma((chunks, 4)),
            dma((chunks, 3)),
            dma,
            dma,
            dma((2, n // 2 - 1)),
            dma((2, n // 2 - 1)),
            dma((2, n // 2)),
            dma((2, n // 2)),
            dma((2,)),
            dma((2,)),
            dma((2,)),
            dma((2,)),
            dma((chunks, 2)),
            dma((chunks, 2)),
            dma((chunks, 2, 2)),
            dma((n // 2, chunks)),
            dma((chunks,)),
            dma((chunks,)),
        ],
        compiler_params=pltpu.CompilerParams(collective_id=0, has_side_effects=True),
    )(
        cotangent,
        expert_ids.reshape(1, -1),
        route_weights.reshape(1, -1),
        gate_pre,
        up_pre,
        down_weight.reshape(chunks, SUB, hidden),
    )
    return weight_grad.reshape(depth, hidden), gate_grad, up_grad


def solution(mesh):
    placed = (
        P(("dp", "expert"), None),
        P(("dp", "expert"), None),
        P(("dp", "expert"), None),
        P("dp", "expert"),
        P("dp", "expert"),
        P("dp", "expert"),
    )
    return jax.shard_map(
        per_device,
        mesh=mesh,
        in_specs=placed,
        out_specs=(P("dp", "expert"), P("dp", "expert"), P("dp", "expert")),
        check_vma=False,
    )
```
